32 devices in a mesh: img: 8 (over z, y), sp: 4 (over x, core).
Axes of the slice: x: 2, y: 2, z: 4, core: 2. Of those that a mesh axis runs over, the one named last changes fastest.
Arguments:
- patches: bfloat16 [4096, 1280], P(('img', 'sp')), parts along dimension 0, may hold values from -6 to 6
- pos_ids: int32 [2, 4096], P(None, 'img'), parts along dimension 1, may hold values from 0 to 31, as said below
- norm_gain: float32 [1280], replicated, may hold values from 0.5 to 1.5
- norm_bias: float32 [1280], replicated, may hold values from -3 to 3
- qkv_weight: bfloat16 [1280, 3, 1280], P(None, None, 'sp')
- qkv_bias: float32 [3, 1280], replicated, may hold values from -3 to 3
- proj_weight: bfloat16 [1280, 1280], P('sp'), may hold values from -0.15625 to 0.15625
- proj_bias: float32 [1280], replicated, may hold values from -3 to 3
- merge_gain: float32 [1280], replicated, may hold values from 0.5 to 1.5
- merge_bias: float32 [1280], replicated, may hold values from -3 to 3
- fc1_weight: bfloat16 [5120, 5120], P(None, 'sp'), may hold values from -0.078125 to 0.078125
- fc1_bias: float32 [5120], P('sp'), may hold values from -3 to 3
Outputs:
- vit_out: bfloat16 [4096, 1280], P(('img', 'sp')), parts along dimension 0
- merged_hidden: bfloat16 [1024, 5120], P('img', 'sp'), parts along dimension 0
The draws below stay inside these ranges and needn't reach their ends.
There are 8 independent parts, one for each index of `img`. The reference program is written for one: setup_inputs(seed, part) draws one part's arguments, and reference() takes and returns one part's arrays. A program takes and returns all parts, laid end to end along the dimension named above; an argument that names none is the same for every part. Nothing has to cross between parts.
Inputs may be any that keep to these rules, and one draw needn't show every extreme that they name: pos_ids[0] and pos_ids[1] are the row and column of each patch on a grid of 2 R by 2 C patches, where the grid of 2x2 blocks has R rows and C columns, R C = 128, and one of R and C equals min(8, 128); each aligned run of 4 patches is one 2x2 block in row-major order inside it; every block of the grid appears once, in the order that the argument gives.
All inputs are finite; a program needn't handle non-finite values.
Results may differ from the reference program's by a relative error of at most 0.006.
Values may be sent and summed in bfloat16 or wider, within the bound.
A program may use at most 64 MiB of HBM per device.

```python
import jax
import jax.numpy as jnp
from jax import lax

D = 1280
HEADS = 16
MERGE_WIDTH = 5120
PATCHES = 512
MERGED = 128


def draw_pos_ids(key, part):
    short_side = min(8, MERGED)
    long_side = MERGED // short_side
    table = jnp.array([short_side, long_side], jnp.int32)
    pick = jax.random.randint(jax.random.fold_in(key, 11), (), 0, 2)
    block_width = table[pick]
    order = jax.random.permutation(jax.random.fold_in(key, 13), MERGED).astype(jnp.int32)
    index = jnp.arange(PATCHES, dtype=jnp.int32)
    block = order[index // 4]
    inner = index % 4
    block_row = block // block_width
    block_col = block % block_width
    row = 2 * block_row + inner // 2
    col = 2 * block_col + inner % 2
    return jnp.stack([row, col]).astype(jnp.int32)


def draw_qkv_weight(key, part):
    base = jax.random.normal(key, (D, 3, D), jnp.float32) / jnp.sqrt(jnp.float32(D))
    return base.astype(jnp.bfloat16)


def block_scale(stream_key, extent, shards, smallest, top_value):
    loudness, own = 1.0, jax.random.fold_in(stream_key, 6)
    for dim, parts in shards:
        heights = jnp.exp(jax.random.uniform(jax.random.fold_in(own, dim), (parts,), jnp.float32, smallest / len(shards), top_value / len(shards)))
        loudness = loudness * jnp.repeat(heights, extent[dim] // parts).reshape([-1 if axis == dim else 1 for axis in range(len(extent))])
    return loudness


def bell_draw(stream_key, dims, spread, reach, cuts=(), held_as=jnp.bfloat16):
    values = jax.random.normal(stream_key, dims, jnp.float32) * spread
    if len(cuts) > 0:
        values = block_scale(stream_key, dims, cuts, -0.22, 0.18) * values
    return jnp.clip(values, min=-reach, max=reach).astype(held_as)


def setup_inputs(seed: int = 0, part: int = 0) -> dict:
    key_of = jax.random.split(jax.random.key(seed), 13)
    part_splits = jax.random.split(jax.random.fold_in(key_of[12], part), 13)
    patches = bell_draw(part_splits[0], (PATCHES, D), 1.0, 6.0, ((0, 4),))
    pos_ids = draw_pos_ids(jax.random.fold_in(jax.random.fold_in(key_of[12], part), 71), part)
    norm_gain = jnp.clip(1.0 + 0.1 * jax.random.normal(key_of[2], (D,), jnp.float32), 0.5, 1.5)
    norm_bias = bell_draw(key_of[3], (D,), 0.5, 3.0, (), jnp.float32)
    qkv_weight = draw_qkv_weight(jax.random.fold_in(key_of[12], 71), part)
    qkv_bias = bell_draw(key_of[5], (3, D), 0.5, 3.0, (), jnp.float32)
    proj_weight = bell_draw(key_of[6], (D, D), D ** -0.5, 0.15625, ((0, 4),))
    proj_bias = bell_draw(key_of[7], (D,), 0.5, 3.0, (), jnp.float32)
    merge_gain = jnp.clip(1.0 + 0.1 * jax.random.normal(key_of[8], (D,), jnp.float32), 0.5, 1.5)
    merge_bias = bell_draw(key_of[9], (D,), 0.5, 3.0, (), jnp.float32)
    fc1_weight = bell_draw(key_of[10], (MERGE_WIDTH, MERGE_WIDTH), MERGE_WIDTH ** -0.5, 0.078125, ((1, 4),))
    fc1_bias = bell_draw(key_of[11], (MERGE_WIDTH,), 0.5, 3.0, ((0, 4),), jnp.float32)
    return dict(patches=patches, pos_ids=pos_ids, norm_gain=norm_gain, norm_bias=norm_bias, qkv_weight=qkv_weight, qkv_bias=qkv_bias, proj_weight=proj_weight, proj_bias=proj_bias, merge_gain=merge_gain, merge_bias=merge_bias, fc1_weight=fc1_weight, fc1_bias=fc1_bias)


def layer_norm(values, gain, bias):
    mean = lax.optimization_barrier(jnp.mean(values, axis=-1, keepdims=True))
    centered = values - mean
    var = lax.optimization_barrier(jnp.mean(centered * centered, axis=-1, keepdims=True))
    return centered * lax.rsqrt(var + 1e-06) * gain + bias

def rotate(values, positions, nheads):
    count = values.shape[0]
    hdim = values.shape[1] // nheads
    quarter = hdim // 4
    inv = 1.0 / 10000.0 ** (jnp.arange(quarter, dtype=jnp.float32) * 2.0 / (hdim // 2))
    rows = positions[0].astype(jnp.float32)[:, None] * inv
    cols = positions[1].astype(jnp.float32)[:, None] * inv
    angle = jnp.concatenate([rows, cols, rows, cols], axis=1)
    cosine = jnp.cos(angle)[:, None, :]
    sine = jnp.sin(angle)[:, None, :]
    shaped = values.reshape(count, nheads, hdim)
    half = hdim // 2
    turned = jnp.concatenate([-shaped[..., half:], shaped[..., :half]], axis=-1)
    return (shaped * cosine + turned * sine).reshape(count, nheads * hdim)

def reference(patches, pos_ids, norm_gain, norm_bias, qkv_weight, qkv_bias, proj_weight, proj_bias, merge_gain, merge_bias, fc1_weight, fc1_bias):
    count = patches.shape[0]
    width = patches.shape[1]
    hdim = width // HEADS
    xfloat = patches.astype(jnp.float32)
    normed = layer_norm(xfloat, norm_gain, norm_bias).astype(jnp.bfloat16)
    qkv = jnp.dot(normed, qkv_weight.reshape(width, 3 * width), preferred_element_type=jnp.float32).reshape(count, 3, width)
    qkv = qkv + qkv_bias[None]
    query = rotate(qkv[:, 0], pos_ids, HEADS).astype(jnp.bfloat16)
    keys = rotate(qkv[:, 1], pos_ids, HEADS).astype(jnp.bfloat16)
    value = qkv[:, 2].astype(jnp.bfloat16)
    qh = query.reshape(count, HEADS, hdim).transpose(1, 0, 2)
    kh = keys.reshape(count, HEADS, hdim).transpose(1, 0, 2)
    vh = value.reshape(count, HEADS, hdim).transpose(1, 0, 2)
    scale = 1.0 / jnp.sqrt(jnp.float32(hdim))

    def one_head(triple):
        qone, kone, vone = triple
        scores = jnp.dot(qone, kone.T, preferred_element_type=jnp.float32) * scale
        top = lax.optimization_barrier(jnp.max(scores, axis=-1, keepdims=True))
        expo = jnp.exp(scores - top)
        weights = (expo / lax.optimization_barrier(jnp.sum(expo, axis=-1, keepdims=True))).astype(jnp.bfloat16)
        return jnp.dot(weights, vone, preferred_element_type=jnp.float32).astype(jnp.bfloat16)
    heads_out = lax.map(one_head, (qh, kh, vh))
    attended = heads_out.transpose(1, 0, 2).reshape(count, width)
    projected = jnp.dot(attended, proj_weight, preferred_element_type=jnp.float32)
    vit_out = (xfloat + projected + proj_bias).astype(jnp.bfloat16)
    zn = layer_norm(vit_out.astype(jnp.float32), merge_gain, merge_bias).astype(jnp.bfloat16)
    blocks = zn.reshape(count // 4, 4 * width)
    hidden = jnp.dot(blocks, fc1_weight, preferred_element_type=jnp.float32) + fc1_bias
    merged_hidden = jax.nn.gelu(hidden, approximate=False).astype(jnp.bfloat16)
    return (vit_out, merged_hidden)
```

```python
import functools

import jax
import jax.numpy as jnp
import numpy as np
from jax import lax
from jax.experimental import pallas as pl
from jax.experimental.pallas import tpu as pltpu
from jax.sharding import PartitionSpec as P

HEADS = 16
MESH = pl.DeviceIdType.MESH
F32 = jnp.float32
BF16 = jnp.bfloat16


def norm_rows(v, gain, bias):
    mean = jnp.mean(v, axis=-1, keepdims=True)
    cen = v - mean
    var = jnp.mean(cen * cen, axis=-1, keepdims=True)
    return cen * lax.rsqrt(var + 1e-06) * gain + bias


def put(ref, row, v):
    for t in range(ref.shape[-3]):
        ref[t, row:row + v.shape[0]] = v[:, t * 128:(t + 1) * 128]


def every_fourth(ref, k, n):
    return jnp.concatenate([ref[t, pl.ds(k, n, stride=4), :] for t in range(ref.shape[-3])], axis=1)


def fused_kernel(
    hdim, x_hbm, pos_ref, inv_ref, g1_ref, b1_ref, wq_hbm, bq_ref, pw_hbm, pb_ref, g2_ref, b2_ref, fw_hbm, fb_ref,
    vit_ref, out_ref,
    xb, xf, nf, nall, wq, pw, fw, tab, bqt, qs, ks, vs, att_t, att, att_in, pf, ps, pr, zb, hid, vf,
    loc, snd, rcv,
):
    me = lax.axis_index("sp")
    chip = me // 2
    core = me % 2
    partner = {"sp": me + 1 - 2 * core}
    peer = {"sp": lax.rem(me + 2, 4)}
    rows, width = x_hbm.shape
    half = rows // 2
    quad = rows // 4
    lw = pw_hbm.shape[0]
    nh = lw // hdim
    hp = qs.shape[2]
    count = 4 * rows
    cols = 2 * rows
    kdim = fw_hbm.shape[0] // 4

    def local(src, dst, i):
        return pltpu.make_async_copy(src, dst, loc.at[i])

    def remote(src, dst, i, dev):
        return pltpu.make_async_remote_copy(
            src_ref=src, dst_ref=dst, send_sem=snd.at[i], recv_sem=rcv.at[i], device_id=dev, device_id_type=MESH
        )

    lx = local(x_hbm, xb.at[0], 0)
    lx.start()
    lq = local(wq_hbm, wq, 1)
    lq.start()
    lp = local(pw_hbm, pw.at[0, pl.ds(0, lw)], 2)
    lp.start()
    lf = [local(fw_hbm.at[pl.ds(k * kdim, kdim)], fw.at[k], 3 + k) for k in range(4)]
    for c in lf:
        c.start()

    barrier = pltpu.get_barrier_semaphore()
    for dev in (partner, peer):
        pl.semaphore_signal(barrier, inc=1, device_id=dev, device_id_type=MESH)
    lx.wait()
    pl.semaphore_wait(barrier, 2)

    x_half = [
        remote(xb.at[0, pl.ds(h * half, half)], xb.at[2, pl.ds(h * half, half)], 1 + h, peer) for h in range(2)
    ]
    for c in x_half:
        c.start()
    x_part = remote(xb.at[0], xb.at[1], 0, partner)
    x_part.start()
    fwd = [
        remote(xb.at[2, pl.ds(h * half, half)], xb.at[3, pl.ds(h * half, half)], 3 + h, partner) for h in range(2)
    ]

    slot_c = lax.broadcasted_iota(jnp.int32, (count, count), 1)
    side = slot_c // cols
    rest = slot_c % cols
    kk = rest // half
    cc = (rest % half) // quad
    bb = rest % quad
    ch = jnp.where(side == 0, chip, 1 - chip)
    want = ((2 * ch + cc) * quad + bb) * 4 + kk
    hot = (want == lax.broadcasted_iota(jnp.int32, (count, count), 0)).astype(F32).astype(BF16)
    tab[0, 0:8] = jnp.zeros((8, count), F32)
    tab[0, 0:2] = pos_ref[...].astype(F32)
    pos = jnp.dot(tab[0, 0:8].astype(BF16), hot, preferred_element_type=F32)
    th = hdim // 2
    invc = jnp.transpose(inv_ref[...])
    angle = invc[0:th, 0:1] * pos[0:1, :] + invc[0:th, 1:2] * pos[1:2, :]
    tab[0] = jnp.cos(angle)
    tab[1] = jnp.sin(angle)
    bqt[...] = jnp.zeros(bqt.shape, F32)
    bqt[0:3] = bq_ref[...]
    turned = pltpu.roll(bqt[0:8], lax.rem(width - me * lw, width), 1)
    bqt[0:8] = turned
    lwp = att_t.shape[0]
    bias_t = jnp.transpose(bqt[:, 0:lwp])
    att_t[...] = jnp.zeros(att_t.shape, F32)
    pw[0, lw:lwp] = jnp.zeros((lwp - lw, width), BF16)
    pw[1, lw:lwp] = jnp.zeros((lwp - lw, width), BF16)
    hid[...] = jnp.zeros(hid.shape, F32)
    g1 = g1_ref[...].reshape(1, width)
    b1 = b1_ref[...].reshape(1, width)

    def norm_half(slot, h):
        v = xb[slot, h * half:(h + 1) * half].astype(F32)
        if slot % 2 == 0:
            put(xf.at[slot // 2], h * half, v)
        put(nf, 0, norm_rows(v, g1, b1))
        at = core if slot % 2 == 0 else 1 - core
        for k in range(4):
            piece = every_fourth(nf, k, half // 4).astype(BF16)
            start = pl.multiple_of((slot // 2) * cols + k * half + at * quad + h * (quad // 2), quad // 2)
            nall[pl.ds(start, quad // 2), :] = piece

    def qkv_side(s):
        n = nall[s * cols:(s + 1) * cols]
        cos = tab[0, :, s * cols:(s + 1) * cols]
        sin = tab[1, :, s * cols:(s + 1) * cols]
        for c in range(3):
            res = lax.dot_general(
                wq[c * lw:(c + 1) * lw], n, (((1,), (1,)), ((), ())), preferred_element_type=F32
            ) + bias_t[0:lw, c:c + 1]
            for h in range(nh):
                a = res[h * hdim:h * hdim + th]
                b = res[h * hdim + th:(h + 1) * hdim]
                if c == 2:
                    vs[h, :, s * cols:(s + 1) * cols] = res[h * hdim:(h + 1) * hdim].astype(BF16)
                    continue
                full = jnp.concatenate(
                    [a * cos - b * sin, b * cos + a * sin, jnp.zeros((hp - hdim, cols), F32)], axis=0
                )
                if c == 0:
                    for m in range(2):
                        qs[m, h, :, s * rows:(s + 1) * rows] = full[:, m * rows:(m + 1) * rows].astype(BF16)
                else:
                    ks[h, s * cols:(s + 1) * cols] = jnp.transpose(full).astype(BF16)

    norm_half(0, 0)
    norm_half(0, 1)
    lp.wait()
    p_send = remote(pw.at[0, pl.ds(0, lw)], pw.at[1, pl.ds(0, lw)], 7, partner)
    p_send.start()
    x_part.wait_recv()
    norm_half(1, 0)
    norm_half(1, 1)
    lq.wait()
    qkv_side(0)
    for h in range(2):
        x_half[h].wait_recv()
        fwd[h].start()
        norm_half(2, h)
    for h in range(2):
        fwd[h].wait_recv()
        norm_half(3, h)
    qkv_side(1)

    scale = 1.0 / np.sqrt(np.float32(hdim))

    def att_copy(m):
        return remote(att.at[m], att_in.at[m], 5 + m, partner)

    def attend(m, _):
        for h in range(nh):
            s = jnp.dot(ks[h], qs[m, h], preferred_element_type=F32) * scale
            e = jnp.exp(s - jnp.max(s, axis=0, keepdims=True))
            w = (e / jnp.sum(e, axis=0, keepdims=True)).astype(BF16)
            att_t[h * hdim:(h + 1) * hdim] = jnp.dot(vs[h], w, preferred_element_type=F32)
        att[m] = jnp.transpose(att_t[...]).astype(BF16)
        att_copy(m).start()
        return 0

    lax.fori_loop(0, 2, attend, 0)
    p_send.wait_recv()

    def part_copy(k):
        return remote(ps.at[k], pr.at[k], 8 + k, peer)

    def project(k, _):
        m = k // 2

        @pl.when(k % 2 == 0)
        def _():
            att_copy(m).wait_recv()

        base = (k % 2) * half + core * quad
        near = pl.ds(pl.multiple_of(base, quad), quad)
        far = pl.ds(pl.multiple_of(rows + base, quad), quad)
        mine = jnp.concatenate([att[m, near], att[m, far]], axis=0)
        theirs = jnp.concatenate([att_in[m, near], att_in[m, far]], axis=0)
        res = jnp.dot(mine, pw[0], preferred_element_type=F32) + jnp.dot(theirs, pw[1], preferred_element_type=F32)
        pf[k] = res
        ps[k, pl.ds(pl.multiple_of(chip * quad, quad), quad)] = res[0:quad].astype(BF16)
        ps[k, pl.ds(pl.multiple_of((1 - chip) * quad, quad), quad)] = res[quad:].astype(BF16)
        part_copy(k).start()
        return 0

    lax.fori_loop(0, 4, project, 0)
    pb = pb_ref[...].reshape(1, width)
    g2 = g2_ref[...].reshape(1, width)
    b2 = b2_ref[...].reshape(1, width)

    def z_copy(k):
        mine = pl.ds(pl.multiple_of(core * half, half), half)
        return remote(zb.at[k, mine], zb.at[k, mine], 12 + k, partner)

    def finish(k, _):
        @pl.when(k < 4)
        def _():
            part_copy(k).wait_recv()
            for s in range(2):
                at = chip if s == 0 else 1 - chip
                got = pr[k, pl.ds(pl.multiple_of(at * quad, quad), quad)].astype(F32)
                v = every_fourth(xf.at[s], k, quad) + (pf[k, s * quad:(s + 1) * quad] + got) + pb
                v = v.astype(BF16).astype(F32)
                if s == 0:
                    for t in range(vf.shape[0]):
                        vf[t, pl.ds(k, quad, stride=4), :] = v[:, t * 128:(t + 1) * 128]
                z = norm_rows(v, g2, b2).astype(BF16)
                zb[k, pl.ds(pl.multiple_of(core * half + at * quad, quad), quad)] = z
            z_copy(k).start()

        @pl.when(k > 0)
        def _():
            z_copy(k - 1).wait_recv()
            pltpu.make_async_copy(fw_hbm.at[pl.ds(0, kdim)], fw.at[k - 1], loc.at[3 + k - 1]).wait()
            hid[...] += jnp.dot(zb[k - 1], fw[k - 1], preferred_element_type=F32)

        return 0

    lax.fori_loop(0, 5, finish, 0)
    for t in range(vf.shape[0]):
        vit_ref[:, t * 128:(t + 1) * 128] = vf[t].astype(BF16)
    h = hid[...] + fb_ref[...].reshape(1, width)
    res = (0.5 * h * (1.0 + lax.erf(h * np.float32(np.sqrt(0.5))))).astype(BF16)
    for c in range(2):
        for p in range(2):
            out_ref[(2 * p + c) * quad:(2 * p + c + 1) * quad] = res[(2 * c + p) * quad:(2 * c + p + 1) * quad]
    x_part.wait_send()
    p_send.wait_send()
    for c in x_half + fwd:
        c.wait_send()
    for m in range(2):
        att_copy(m).wait_send()
    for k in range(4):
        part_copy(k).wait_send()
        z_copy(k).wait_send()


def fused(patches, pos_ids, norm_gain, norm_bias, qkv_weight, qkv_bias, proj_weight, proj_bias,
          merge_gain, merge_bias, fc1_weight, fc1_bias):
    rows, width = patches.shape
    hdim = width // HEADS
    lw = proj_weight.shape[0]
    nh = lw // hdim
    hp = -(-hdim // 128) * 128
    lwp = -(-lw // 128) * 128
    half, quad, count = rows // 2, rows // 4, 4 * rows
    hidden = fc1_weight.shape[1]
    quarter = hdim // 4
    steps = 1.0 / np.float32(10000.0) ** (np.arange(quarter, dtype=np.float32) * np.float32(2.0) / (hdim // 2))
    inv = np.zeros((128, 128), np.float32)
    inv[0, :quarter] = steps
    inv[1, quarter:2 * quarter] = steps
    wq = jnp.transpose(qkv_weight, (1, 2, 0)).reshape(3 * lw, width)
    vm = pl.BlockSpec(memory_space=pltpu.VMEM)
    hbm = pl.BlockSpec(memory_space=pl.ANY)
    V = pltpu.VMEM
    return pl.pallas_call(
        functools.partial(fused_kernel, hdim),
        out_shape=(jax.ShapeDtypeStruct((rows, width), BF16), jax.ShapeDtypeStruct((rows, hidden), BF16)),
        in_specs=[hbm, vm, vm, vm, vm, hbm, vm, hbm, vm, vm, vm, hbm, vm],
        out_specs=(vm, vm),
        scratch_shapes=[
            V((4, rows, width), BF16),
            V((2, width // 128, rows, 128), F32),
            V((width // 128, half, 128), F32),
            V((count, width), BF16),
            V((3 * lw, width), BF16),
            V((2, lwp, width), BF16),
            V((4, fc1_weight.shape[0] // 4, hidden), BF16),
            V((2, hdim // 2, count), F32),
            V((128, width), F32),
            V((2, nh, hp, 2 * rows), BF16),
            V((nh, count, hp), BF16),
            V((nh, hdim, count), BF16),
            V((lwp, 2 * rows), F32),
            V((2, 2 * rows, lwp), BF16),
            V((2, 2 * rows, lwp), BF16),
            V((4, half, width), F32),
            V((4, half, width), BF16),
            V((4, half, width), BF16),
            V((4, rows, width), BF16),
            V((rows, hidden), F32),
            V((width // 128, rows, 128), F32),
            pltpu.SemaphoreType.DMA((7,)),
            pltpu.SemaphoreType.DMA((16,)),
            pltpu.SemaphoreType.DMA((16,)),
        ],
        compiler_params=pltpu.CompilerParams(
            collective_id=0, has_side_effects=True, vmem_limit_bytes=60 * 1024 * 1024
        ),
    )(patches, pos_ids, jnp.asarray(inv), norm_gain, norm_bias, wq, qkv_bias, proj_weight, proj_bias,
      merge_gain, merge_bias, fc1_weight, fc1_bias)


def layer_norm(values, gain, bias):
    mean = jnp.mean(values, axis=-1, keepdims=True)
    centered = values - mean
    var = jnp.mean(centered * centered, axis=-1, keepdims=True)
    return centered * lax.rsqrt(var + 1e-06) * gain + bias


def rotate(values, positions, nheads):
    count = values.shape[0]
    hdim = values.shape[1] // nheads
    quarter = hdim // 4
    inv = 1.0 / 10000.0 ** (jnp.arange(quarter, dtype=jnp.float32) * 2.0 / (hdim // 2))
    rows = positions[0].astype(jnp.float32)[:, None] * inv
    cols = positions[1].astype(jnp.float32)[:, None] * inv
    angle = jnp.concatenate([rows, cols, rows, cols], axis=1)
    cosine = jnp.cos(angle)[:, None, :]
    sine = jnp.sin(angle)[:, None, :]
    shaped = values.reshape(count, nheads, hdim)
    half = hdim // 2
    turned = jnp.concatenate([-shaped[..., half:], shaped[..., :half]], axis=-1)
    return (shaped * cosine + turned * sine).reshape(count, nheads * hdim)


def attend(query, keys, value, nheads, hdim):
    count = query.shape[0]
    block = min(512, count)
    qblocks = query.reshape(count // block, block, nheads, hdim)
    kshaped = keys.reshape(count, nheads, hdim)
    vshaped = value.reshape(count, nheads, hdim)
    scale = 1.0 / jnp.sqrt(jnp.float32(hdim))

    def one_block(qpart):
        scores = (
            jnp.einsum("bhd,khd->hbk", qpart, kshaped, preferred_element_type=jnp.float32) * scale
        )
        top = jnp.max(scores, axis=-1, keepdims=True)
        expo = jnp.exp(scores - top)
        weights = (expo / jnp.sum(expo, axis=-1, keepdims=True)).astype(jnp.bfloat16)
        result = jnp.einsum("hbk,khd->bhd", weights, vshaped, preferred_element_type=jnp.float32)
        return result.astype(jnp.bfloat16).reshape(block, nheads * hdim)

    return lax.map(one_block, qblocks).reshape(count, nheads * hdim)


def per_device(
    patches,
    pos_ids,
    norm_gain,
    norm_bias,
    qkv_weight,
    qkv_bias,
    proj_weight,
    proj_bias,
    merge_gain,
    merge_bias,
    fc1_weight,
    fc1_bias,
):
    groups = lax.axis_size("sp")
    where = lax.axis_index("sp")
    prow = patches.shape[0]
    width = patches.shape[1]
    heads_local = HEADS // groups
    hdim = width // HEADS
    local_width = width // groups
    xfloat = patches.astype(jnp.float32)
    normed = layer_norm(xfloat, norm_gain, norm_bias).astype(jnp.bfloat16)
    bias_local = lax.dynamic_slice_in_dim(qkv_bias, where * local_width, local_width, 1)
    qkv = (
        jnp.einsum(
            "pd,dcn->pcn",
            lax.all_gather(normed, "sp", axis=0, tiled=True),
            qkv_weight,
            preferred_element_type=jnp.float32,
        )
        + bias_local[None]
    )
    query = rotate(qkv[:, 0], pos_ids, heads_local).astype(jnp.bfloat16)
    keys = rotate(qkv[:, 1], pos_ids, heads_local).astype(jnp.bfloat16)
    value = qkv[:, 2].astype(jnp.bfloat16)
    spread = jnp.stack([query, keys, value])
    attended = attend(spread[0], spread[1], spread[2], heads_local, hdim)
    returned = lax.all_to_all(attended, "sp", split_axis=0, concat_axis=1, tiled=True)
    projected = jnp.dot(
        returned,
        lax.all_gather(proj_weight, "sp", axis=0, tiled=True),
        preferred_element_type=jnp.float32,
    )
    vit_out = (xfloat + projected + proj_bias).astype(jnp.bfloat16)
    zn = layer_norm(vit_out.astype(jnp.float32), merge_gain, merge_bias).astype(jnp.bfloat16)
    blocks = zn.reshape(prow // 4, 4 * width)
    hidden = (
        jnp.dot(
            lax.all_gather(blocks, "sp", axis=0, tiled=True),
            fc1_weight,
            preferred_element_type=jnp.float32,
        )
        + fc1_bias
    )
    merged_hidden = jax.nn.gelu(hidden, approximate=False).astype(jnp.bfloat16)
    return (vit_out, merged_hidden)


def solution(mesh):
    body = fused if mesh.shape["sp"] == 4 else per_device
    return jax.shard_map(
        body,
        mesh=mesh,
        in_specs=(
            P(("img", "sp"), None),
            P(None, "img"),
            P(),
            P(),
            P(None, None, "sp"),
            P(),
            P("sp", None),
            P(),
            P(),
            P(),
            P(None, "sp"),
            P("sp"),
        ),
        out_specs=(P(("img", "sp"), None), P("img", "sp")),
        check_vma=False,
    )
```

```python
import functools

import jax
import jax.numpy as jnp
import numpy as np
from jax import lax
from jax.experimental import pallas as pl
from jax.experimental.pallas import tpu as pltpu
from jax.sharding import PartitionSpec as P

HEADS = 16
MESH = pl.DeviceIdType.MESH
F32 = jnp.float32
BF16 = jnp.bfloat16
VM_LIMIT = 56 * 1024 * 1024


def norm_rows(v, gain, bias):
    mean = jnp.mean(v, axis=-1, keepdims=True)
    cen = v - mean
    var = jnp.mean(cen * cen, axis=-1, keepdims=True)
    return cen * lax.rsqrt(var + 1e-06) * gain + bias


def put(ref, row, v):
    for t in range(ref.shape[-3]):
        ref[t, row:row + v.shape[0]] = v[:, t * 128:(t + 1) * 128]


def every_fourth(ref, k, n):
    return jnp.concatenate([ref[t, pl.ds(k, n, stride=4), :] for t in range(ref.shape[-3])], axis=1)


def fused_kernel(
    hdim, x_hbm, pos_ref, inv_ref, g1_ref, b1_ref, wq_hbm, bq_ref, pw_hbm, pb_ref, g2_ref, b2_ref, fw_hbm, fb_ref,
    vit_ref, out_ref,
    xb, xf, nf, nall, wq, pw, fw, tab, bqt, qs, ks, vs, att_t, att, att_in, pf, ps, pr, zb, hid, vf,
    loc, snd, rcv,
):
    me = lax.axis_index("sp")
    scale = np.float32(np.log2(np.e) / np.sqrt(hdim))
    chip = me // 2
    core = me % 2
    partner = {"sp": me + 1 - 2 * core}
    peer = {"sp": lax.rem(me + 2, 4)}
    rows, width = x_hbm.shape
    half = rows // 2
    quad = rows // 4
    lw = pw_hbm.shape[0]
    nh = lw // hdim
    hp = qs.shape[2]
    count = 4 * rows
    cols = 2 * rows
    kdim = fw_hbm.shape[0] // 4

    def local(src, dst, i):
        return pltpu.make_async_copy(src, dst, loc.at[i])

    def remote(src, dst, i, dev):
        return pltpu.make_async_remote_copy(
            src_ref=src, dst_ref=dst, send_sem=snd.at[i], recv_sem=rcv.at[i], device_id=dev, device_id_type=MESH
        )

    lx = local(x_hbm, xb.at[0], 0)
    lx.start()
    lq = local(wq_hbm, wq, 1)
    lq.start()
    lp = local(pw_hbm, pw.at[0, pl.ds(0, lw)], 2)
    lp.start()
    lf = [local(fw_hbm.at[pl.ds(k * kdim, kdim)], fw.at[k], 3 + k) for k in range(4)]
    for c in lf:
        c.start()

    barrier = pltpu.get_barrier_semaphore()
    for dev in (partner, peer):
        pl.semaphore_signal(barrier, inc=1, device_id=dev, device_id_type=MESH)
    lx.wait()
    pl.semaphore_wait(barrier, 2)

    x_half = [
        remote(xb.at[0, pl.ds(h * half, half)], xb.at[2, pl.ds(h * half, half)], 1 + h, peer) for h in range(2)
    ]
    for c in x_half:
        c.start()
    x_part = remote(xb.at[0], xb.at[1], 0, partner)
    x_part.start()
    fwd = [
        remote(xb.at[2, pl.ds(h * half, half)], xb.at[3, pl.ds(h * half, half)], 3 + h, partner) for h in range(2)
    ]

    slot_c = lax.broadcasted_iota(jnp.int32, (count, count), 1)
    side = slot_c // cols
    rest = slot_c % cols
    kk = rest // half
    cc = (rest % half) // quad
    bb = rest % quad
    ch = jnp.where(side == 0, chip, 1 - chip)
    want = ((2 * ch + cc) * quad + bb) * 4 + kk
    hot = (want == lax.broadcasted_iota(jnp.int32, (count, count), 0)).astype(F32).astype(BF16)
    tab[0, 0:8] = jnp.zeros((8, count), F32)
    tab[0, 0:2] = pos_ref[...].astype(F32)
    pos = jnp.dot(tab[0, 0:8].astype(BF16), hot, preferred_element_type=F32)
    th = hdim // 2
    invc = jnp.transpose(inv_ref[...])
    angle = invc[0:th, 0:1] * pos[0:1, :] + invc[0:th, 1:2] * pos[1:2, :]
    tab[0] = jnp.cos(angle)
    tab[1] = jnp.sin(angle)
    bqt[...] = jnp.zeros(bqt.shape, F32)
    bqt[0:3] = bq_ref[...]
    turned = pltpu.roll(bqt[0:8], lax.rem(width - me * lw, width), 1)
    bqt[0:8] = turned
    lwp = att_t.shape[0]
    bias_t = jnp.transpose(bqt[:, 0:lwp])
    att_t[...] = jnp.zeros(att_t.shape, F32)
    for h in range(nh):
        vs[h, hdim:] = jnp.ones((vs.shape[1] - hdim, count), BF16)
    pw[0, lw:lwp] = jnp.zeros((lwp - lw, width), BF16)
    pw[1, lw:lwp] = jnp.zeros((lwp - lw, width), BF16)
    hid[...] = jnp.zeros(hid.shape, F32)
    g1 = g1_ref[...].reshape(1, width)
    b1 = b1_ref[...].reshape(1, width)

    def norm_half(slot, h):
        v = xb[slot, h * half:(h + 1) * half].astype(F32)
        if slot % 2 == 0:
            put(xf.at[slot // 2], h * half, v)
        put(nf, 0, norm_rows(v, g1, b1))
        at = core if slot % 2 == 0 else 1 - core
        for k in range(4):
            piece = every_fourth(nf, k, half // 4).astype(BF16)
            start = pl.multiple_of((slot // 2) * cols + k * half + at * quad + h * (quad // 2), quad // 2)
            nall[pl.ds(start, quad // 2), :] = piece

    def qkv_side(s):
        n = nall[s * cols:(s + 1) * cols]
        cos = tab[0, :, s * cols:(s + 1) * cols]
        sin = tab[1, :, s * cols:(s + 1) * cols]
        for c in range(3):
            res = lax.dot_general(
                wq[c * lw:(c + 1) * lw], n, (((1,), (1,)), ((), ())), preferred_element_type=F32
            ) + bias_t[0:lw, c:c + 1]
            for h in range(nh):
                a = res[h * hdim:h * hdim + th]
                b = res[h * hdim + th:(h + 1) * hdim]
                if c == 2:
                    vs[h, 0:hdim, s * cols:(s + 1) * cols] = res[h * hdim:(h + 1) * hdim].astype(BF16)
                    continue
                full = jnp.concatenate(
                    [a * cos - b * sin, b * cos + a * sin, jnp.zeros((hp - hdim, cols), F32)], axis=0
                )
                if c == 0:
                    full = full * scale
                    for k in range(4):
                        qs[k, h, :, s * half:(s + 1) * half] = full[:, k * half:(k + 1) * half].astype(BF16)
                else:
                    ks[h, s * cols:(s + 1) * cols] = jnp.transpose(full).astype(BF16)

    norm_half(0, 0)
    norm_half(0, 1)
    lp.wait()
    p_send = remote(pw.at[0, pl.ds(0, lw)], pw.at[1, pl.ds(0, lw)], 9, partner)
    p_send.start()
    x_part.wait_recv()
    norm_half(1, 0)
    norm_half(1, 1)
    lq.wait()
    qkv_side(0)
    for h in range(2):
        x_half[h].wait_recv()
        fwd[h].start()
        norm_half(2, h)
        fwd[h].wait_recv()
        norm_half(3, h)
    qkv_side(1)

    def att_copy(m):
        return remote(att.at[m], att_in.at[m], 5 + m, partner)

    def attend(m):
        for h in range(nh):
            s = jnp.dot(ks[h], qs[m, h], preferred_element_type=F32)
            e = jnp.exp2(s - jnp.max(s, axis=0, keepdims=True)).astype(BF16)
            av = jnp.dot(vs[h], e, preferred_element_type=F32)
            att_t[h * hdim:(h + 1) * hdim] = av[0:hdim] * (1.0 / av[hdim:hdim + 1])
        att[m] = jnp.transpose(att_t[...]).astype(BF16)
        att_copy(m).start()

    p_send.wait_recv()

    def part_copy(k):
        return remote(ps.at[k], pr.at[k], 10 + k, peer)

    def project(k):
        att_copy(k).wait_recv()
        near = pl.ds(pl.multiple_of(core * quad, quad), quad)
        far = pl.ds(pl.multiple_of(half + core * quad, quad), quad)
        mine = jnp.concatenate([att[k, near], att[k, far]], axis=0)
        theirs = jnp.concatenate([att_in[k, near], att_in[k, far]], axis=0)
        res = jnp.dot(mine, pw[0], preferred_element_type=F32) + jnp.dot(theirs, pw[1], preferred_element_type=F32)
        pf[k] = res
        ps[k, pl.ds(pl.multiple_of(chip * quad, quad), quad)] = res[0:quad].astype(BF16)
        ps[k, pl.ds(pl.multiple_of((1 - chip) * quad, quad), quad)] = res[quad:].astype(BF16)
        part_copy(k).start()

    def mid(i, _):
        @pl.when(i < 4)
        def _():
            attend(i)

        @pl.when(i > 0)
        def _():
            project(i - 1)

        return 0

    lax.fori_loop(0, 5, mid, 0)
    pb = pb_ref[...].reshape(1, width)
    g2 = g2_ref[...].reshape(1, width)
    b2 = b2_ref[...].reshape(1, width)

    def z_copy(k):
        mine = pl.ds(pl.multiple_of(core * half, half), half)
        return remote(zb.at[k, mine], zb.at[k, mine], 14 + k, partner)

    def finish(k, _):
        @pl.when(k < 4)
        def _():
            part_copy(k).wait_recv()
            for s in range(2):
                at = chip if s == 0 else 1 - chip
                got = pr[k, pl.ds(pl.multiple_of(at * quad, quad), quad)].astype(F32)
                v = every_fourth(xf.at[s], k, quad) + (pf[k, s * quad:(s + 1) * quad] + got) + pb
                v = v.astype(BF16).astype(F32)
                if s == 0:
                    for t in range(vf.shape[0]):
                        vf[t, pl.ds(k, quad, stride=4), :] = v[:, t * 128:(t + 1) * 128]
                z = norm_rows(v, g2, b2).astype(BF16)
                zb[k, pl.ds(pl.multiple_of(core * half + at * quad, quad), quad)] = z
            z_copy(k).start()

        @pl.when(k > 0)
        def _():
            z_copy(k - 1).wait_recv()
            pltpu.make_async_copy(fw_hbm.at[pl.ds(0, kdim)], fw.at[k - 1], loc.at[3 + k - 1]).wait()
            hid[...] += jnp.dot(zb[k - 1], fw[k - 1], preferred_element_type=F32)

        return 0

    lax.fori_loop(0, 5, finish, 0)
    for t in range(vf.shape[0]):
        vit_ref[:, t * 128:(t + 1) * 128] = vf[t].astype(BF16)
    h = hid[...] + fb_ref[...].reshape(1, width)
    res = (0.5 * h * (1.0 + lax.erf(h * np.float32(np.sqrt(0.5))))).astype(BF16)
    for c in range(2):
        for p in range(2):
            out_ref[(2 * p + c) * quad:(2 * p + c + 1) * quad] = res[(2 * c + p) * quad:(2 * c + p + 1) * quad]
    x_part.wait_send()
    p_send.wait_send()
    for c in x_half + fwd:
        c.wait_send()
    for k in range(4):
        att_copy(k).wait_send()
        part_copy(k).wait_send()
        z_copy(k).wait_send()


def put_out(vit, merged, vit_out, merged_out, sems):
    outs = [pltpu.make_async_copy(vit, vit_out, sems.at[0]), pltpu.make_async_copy(merged, merged_out, sems.at[1])]
    for o in outs:
        o.start()
    for o in outs:
        o.wait()


def fused(patches, pos_ids, norm_gain, norm_bias, qkv_weight, qkv_bias, proj_weight, proj_bias,
          merge_gain, merge_bias, fc1_weight, fc1_bias):
    rows, width = patches.shape
    hdim = width // HEADS
    lw = proj_weight.shape[0]
    nh = lw // hdim
    hp = -(-hdim // 128) * 128
    lwp = -(-lw // 128) * 128
    half, quad, count = rows // 2, rows // 4, 4 * rows
    hidden = fc1_weight.shape[1]
    quarter = hdim // 4
    steps = 1.0 / np.float32(10000.0) ** (np.arange(quarter, dtype=np.float32) * np.float32(2.0) / (hdim // 2))
    inv = np.zeros((128, 128), np.float32)
    inv[0, :quarter] = steps
    inv[1, quarter:2 * quarter] = steps
    wq = jnp.transpose(qkv_weight, (1, 2, 0)).reshape(3 * lw, width)
    vm = pl.BlockSpec(memory_space=pltpu.VMEM)
    hbm = pl.BlockSpec(memory_space=pl.ANY)
    V = pltpu.VMEM
    vit, merged = pl.pallas_call(
        functools.partial(fused_kernel, hdim),
        out_shape=(V((rows, width), BF16), V((rows, hidden), BF16)),
        in_specs=[hbm, vm, vm, vm, vm, hbm, vm, hbm, vm, vm, vm, hbm, vm],
        out_specs=(vm, vm),
        scratch_shapes=[
            V((4, rows, width), BF16),
            V((2, width // 128, rows, 128), F32),
            V((width // 128, half, 128), F32),
            V((count, width), BF16),
            V((3 * lw, width), BF16),
            V((2, lwp, width), BF16),
            V((4, fc1_weight.shape[0] // 4, hidden), BF16),
            V((2, hdim // 2, count), F32),
            V((128, width), F32),
            V((4, nh, hp, rows), BF16),
            V((nh, count, hp), BF16),
            V((nh, hdim + 16, count), BF16),
            V((lwp, rows), F32),
            V((4, rows, lwp), BF16),
            V((4, rows, lwp), BF16),
            V((4, half, width), F32),
            V((4, half, width), BF16),
            V((4, half, width), BF16),
            V((4, rows, width), BF16),
            V((rows, hidden), F32),
            V((width // 128, rows, 128), F32),
            pltpu.SemaphoreType.DMA((7,)),
            pltpu.SemaphoreType.DMA((18,)),
            pltpu.SemaphoreType.DMA((18,)),
        ],
        compiler_params=pltpu.CompilerParams(
            collective_id=0, has_side_effects=True, vmem_limit_bytes=VM_LIMIT
        ),
    )(patches, pos_ids, jnp.asarray(inv), norm_gain, norm_bias, wq, qkv_bias, proj_weight, proj_bias,
      merge_gain, merge_bias, fc1_weight, fc1_bias)
    return pl.pallas_call(
        put_out,
        out_shape=(jax.ShapeDtypeStruct(vit.shape, BF16), jax.ShapeDtypeStruct(merged.shape, BF16)),
        in_specs=[vm, vm],
        out_specs=(hbm, hbm),
        scratch_shapes=[pltpu.SemaphoreType.DMA((2,))],
        compiler_params=pltpu.CompilerParams(vmem_limit_bytes=2 * 1024 * 1024),
    )(vit, merged)


def layer_norm(values, gain, bias):
    mean = jnp.mean(values, axis=-1, keepdims=True)
    centered = values - mean
    var = jnp.mean(centered * centered, axis=-1, keepdims=True)
    return centered * lax.rsqrt(var + 1e-06) * gain + bias


def rotate(values, positions, nheads):
    count = values.shape[0]
    hdim = values.shape[1] // nheads
    quarter = hdim // 4
    inv = 1.0 / 10000.0 ** (jnp.arange(quarter, dtype=jnp.float32) * 2.0 / (hdim // 2))
    rows = positions[0].astype(jnp.float32)[:, None] * inv
    cols = positions[1].astype(jnp.float32)[:, None] * inv
    angle = jnp.concatenate([rows, cols, rows, cols], axis=1)
    cosine = jnp.cos(angle)[:, None, :]
    sine = jnp.sin(angle)[:, None, :]
    shaped = values.reshape(count, nheads, hdim)
    half = hdim // 2
    turned = jnp.concatenate([-shaped[..., half:], shaped[..., :half]], axis=-1)
    return (shaped * cosine + turned * sine).reshape(count, nheads * hdim)


def attend(query, keys, value, nheads, hdim):
    count = query.shape[0]
    block = min(512, count)
    qblocks = query.reshape(count // block, block, nheads, hdim)
    kshaped = keys.reshape(count, nheads, hdim)
    vshaped = value.reshape(count, nheads, hdim)
    scale = 1.0 / jnp.sqrt(jnp.float32(hdim))

    def one_block(qpart):
        scores = (
            jnp.einsum("bhd,khd->hbk", qpart, kshaped, preferred_element_type=jnp.float32) * scale
        )
        top = jnp.max(scores, axis=-1, keepdims=True)
        expo = jnp.exp(scores - top)
        weights = (expo / jnp.sum(expo, axis=-1, keepdims=True)).astype(jnp.bfloat16)
        result = jnp.einsum("hbk,khd->bhd", weights, vshaped, preferred_element_type=jnp.float32)
        return result.astype(jnp.bfloat16).reshape(block, nheads * hdim)

    return lax.map(one_block, qblocks).reshape(count, nheads * hdim)


def per_device(
    patches,
    pos_ids,
    norm_gain,
    norm_bias,
    qkv_weight,
    qkv_bias,
    proj_weight,
    proj_bias,
    merge_gain,
    merge_bias,
    fc1_weight,
    fc1_bias,
):
    groups = lax.axis_size("sp")
    where = lax.axis_index("sp")
    prow = patches.shape[0]
    width = patches.shape[1]
    heads_local = HEADS // groups
    hdim = width // HEADS
    local_width = width // groups
    xfloat = patches.astype(jnp.float32)
    normed = layer_norm(xfloat, norm_gain, norm_bias).astype(jnp.bfloat16)
    bias_local = lax.dynamic_slice_in_dim(qkv_bias, where * local_width, local_width, 1)
    qkv = (
        jnp.einsum(
            "pd,dcn->pcn",
            lax.all_gather(normed, "sp", axis=0, tiled=True),
            qkv_weight,
            preferred_element_type=jnp.float32,
        )
        + bias_local[None]
    )
    query = rotate(qkv[:, 0], pos_ids, heads_local).astype(jnp.bfloat16)
    keys = rotate(qkv[:, 1], pos_ids, heads_local).astype(jnp.bfloat16)
    value = qkv[:, 2].astype(jnp.bfloat16)
    spread = jnp.stack([query, keys, value])
    attended = attend(spread[0], spread[1], spread[2], heads_local, hdim)
    returned = lax.all_to_all(attended, "sp", split_axis=0, concat_axis=1, tiled=True)
    projected = jnp.dot(
        returned,
        lax.all_gather(proj_weight, "sp", axis=0, tiled=True),
        preferred_element_type=jnp.float32,
    )
    vit_out = (xfloat + projected + proj_bias).astype(jnp.bfloat16)
    zn = layer_norm(vit_out.astype(jnp.float32), merge_gain, merge_bias).astype(jnp.bfloat16)
    blocks = zn.reshape(prow // 4, 4 * width)
    hidden = (
        jnp.dot(
            lax.all_gather(blocks, "sp", axis=0, tiled=True),
            fc1_weight,
            preferred_element_type=jnp.float32,
        )
        + fc1_bias
    )
    merged_hidden = jax.nn.gelu(hidden, approximate=False).astype(jnp.bfloat16)
    return (vit_out, merged_hidden)


def solution(mesh):
    body = fused if mesh.shape["sp"] == 4 else per_device
    return jax.shard_map(
        body,
        mesh=mesh,
        in_specs=(
            P(("img", "sp"), None),
            P(None, "img"),
            P(),
            P(),
            P(None, None, "sp"),
            P(),
            P("sp", None),
            P(),
            P(),
            P(),
            P(None, "sp"),
            P("sp"),
        ),
        out_specs=(P(("img", "sp"), None), P("img", "sp")),
        check_vma=False,
    )
```
